32 devices in a mesh: dp: 1 (over z), col: 4 (over y), row: 8 (over x, core).
Axes of the slice: x: 4, y: 4, z: 1, core: 2. Of those that a mesh axis runs over, the one named last changes fastest.
The devices are a block of a 4x4x8 slice.
Arguments:
- x_norm: bfloat16 [4096, 2048], P(('dp', 'row'), 'col')
- grad_y: bfloat16 [4096, 2048], P(('dp', 'row'), 'col')
- w_gate: bfloat16 [2048, 16384], P('row', 'col')
- w_up: bfloat16 [2048, 16384], P('row', 'col')
- w_out: bfloat16 [16384, 2048], P('row', 'col')
Outputs:
- output 1: bfloat16 [4096, 2048], P(('dp', 'row'), 'col')
- output 2: float32 [2048, 16384], P(('dp', 'row'), 'col')
- output 3: float32 [2048, 16384], P(('dp', 'row'), 'col')
- output 4: float32 [16384, 2048], P(('dp', 'row'), 'col')
All inputs are finite; a program needn't handle non-finite values.
Results may differ from the reference program's by a relative error of at most 0.0087411.
Values are sent between devices in bfloat16 or wider.
A program may use at most 768 MiB of HBM per device.

```python
import math
import jax
import jax.numpy as jnp
from jax import lax

D_MODEL = 2048
D_FF = 16384
TOKENS = 4096
ROW_BLOCK = min(TOKENS, 1024)
BLOCK_COUNT = TOKENS // ROW_BLOCK
GELU_SCALE = math.sqrt(2.0 / math.pi)


def gelu_pair(pre_act):
    pre_f32 = pre_act.astype(jnp.float32)
    inner_arg = GELU_SCALE * (pre_f32 + 0.044715 * pre_f32 * pre_f32 * pre_f32)
    tanh_val = jnp.tanh(inner_arg)
    gelu_val = 0.5 * pre_f32 * (1.0 + tanh_val)
    gelu_der = 0.5 * (1.0 + tanh_val) + 0.5 * pre_f32 * (1.0 - tanh_val * tanh_val) * GELU_SCALE * (1.0 + 3.0 * 0.044715 * pre_f32 * pre_f32)
    return gelu_val, gelu_der


def setup_inputs(seed: int = 0, part: int = 0) -> dict:
    key_list = jax.random.split(jax.random.key(seed), 4)
    part_key = jax.random.fold_in(key_list[0], part)
    key_x, key_gy = jax.random.split(part_key, 2)
    x_norm = jax.random.normal(key_x, (TOKENS, D_MODEL), jnp.float32).astype(jnp.bfloat16)
    grad_y = jax.random.normal(key_gy, (TOKENS, D_MODEL), jnp.float32).astype(jnp.bfloat16)
    w_gate = (jax.random.normal(key_list[1], (D_MODEL, D_FF), jnp.float32) * D_MODEL ** -0.5).astype(jnp.bfloat16)
    w_up = (jax.random.normal(key_list[2], (D_MODEL, D_FF), jnp.float32) * D_MODEL ** -0.5).astype(jnp.bfloat16)
    w_out = (jax.random.normal(key_list[3], (D_FF, D_MODEL), jnp.float32) * D_FF ** -0.5).astype(jnp.bfloat16)
    return {"x_norm": x_norm, "grad_y": grad_y, "w_gate": w_gate, "w_up": w_up, "w_out": w_out}


def reference(x_norm, grad_y, w_gate, w_up, w_out):
    x_blocks = x_norm.reshape(BLOCK_COUNT, ROW_BLOCK, D_MODEL)
    gy_blocks = grad_y.reshape(BLOCK_COUNT, ROW_BLOCK, D_MODEL)

    def block_step(acc_state, blk_pair):
        acc_gate, acc_up, acc_out = acc_state
        x_blk, gy_blk = blk_pair
        pre_gate = jnp.dot(x_blk, w_gate, preferred_element_type=jnp.float32).astype(jnp.bfloat16)
        pre_up = jnp.dot(x_blk, w_up, preferred_element_type=jnp.float32).astype(jnp.bfloat16)
        gelu_val, gelu_der = gelu_pair(pre_gate)
        up_f32 = pre_up.astype(jnp.float32)
        hidden = (gelu_val * up_f32).astype(jnp.bfloat16)
        grad_h = jnp.dot(gy_blk, w_out.T, preferred_element_type=jnp.float32)
        grad_gate = (grad_h * up_f32 * gelu_der).astype(jnp.bfloat16)
        grad_up = (grad_h * gelu_val).astype(jnp.bfloat16)
        grad_x = (jnp.dot(grad_gate, w_gate.T, preferred_element_type=jnp.float32) + jnp.dot(grad_up, w_up.T, preferred_element_type=jnp.float32)).astype(jnp.bfloat16)
        acc_gate = acc_gate + jnp.dot(x_blk.T, grad_gate, preferred_element_type=jnp.float32)
        acc_up = acc_up + jnp.dot(x_blk.T, grad_up, preferred_element_type=jnp.float32)
        acc_out = acc_out + jnp.dot(hidden.T, gy_blk, preferred_element_type=jnp.float32)
        return (acc_gate, acc_up, acc_out), grad_x

    zero_state = (jnp.zeros((D_MODEL, D_FF), jnp.float32), jnp.zeros((D_MODEL, D_FF), jnp.float32), jnp.zeros((D_FF, D_MODEL), jnp.float32))
    grads, gx_blocks = lax.scan(block_step, zero_state, (x_blocks, gy_blocks))
    dw_gate, dw_up, dw_out = grads
    return gx_blocks.reshape(TOKENS, D_MODEL), dw_gate, dw_up, dw_out
```

```python
import math
import jax
import jax.numpy as jnp
from jax import lax
from jax.sharding import PartitionSpec as P

GELU_SCALE = math.sqrt(2.0 / math.pi)
ROW_DIMS = (((1,), (1,)), ((), ()))
COL_DIMS = (((0,), (0,)), ((), ()))


def gelu_pair(pre_act):
    pre_f32 = pre_act.astype(jnp.float32)
    inner_arg = GELU_SCALE * (pre_f32 + 0.044715 * pre_f32 * pre_f32 * pre_f32)
    tanh_val = jnp.tanh(inner_arg)
    gelu_val = 0.5 * pre_f32 * (1.0 + tanh_val)
    gelu_der = 0.5 * (1.0 + tanh_val) + 0.5 * pre_f32 * (1.0 - tanh_val * tanh_val) * GELU_SCALE * (1.0 + 3.0 * 0.044715 * pre_f32 * pre_f32)
    return gelu_val, gelu_der


def solution(mesh):
    act_spec = P(("dp", "row"), "col")
    weight_spec = P("row", "col")
    n_row, n_col = mesh.shape["row"], mesh.shape["col"]

    to_slice, from_slice = [], []
    for r in range(n_row):
        for c in range(n_col):
            k = r * n_col + c
            dst = (k // n_row) * n_row + k % n_row
            to_slice.append((c * n_row + r, dst))
            from_slice.append((dst, c * n_row + r))

    def block_backward(x_blk, gy_blk, gate_blk, up_blk, out_blk):
        gate = lax.all_to_all(gate_blk, "row", split_axis=1, concat_axis=0, tiled=True)
        up = lax.all_to_all(up_blk, "row", split_axis=1, concat_axis=0, tiled=True)
        out = lax.all_to_all(out_blk, "col", split_axis=0, concat_axis=1, tiled=True)
        out = lax.ppermute(out, ("col", "row"), to_slice)
        x_all = lax.all_gather(lax.all_gather(x_blk, "col", axis=1, tiled=True), "row", axis=0, tiled=True)
        gy_all = lax.all_gather(lax.all_gather(gy_blk, "col", axis=1, tiled=True), "row", axis=0, tiled=True)
        pre_gate = jnp.dot(x_all, gate, preferred_element_type=jnp.float32).astype(jnp.bfloat16)
        pre_up = jnp.dot(x_all, up, preferred_element_type=jnp.float32).astype(jnp.bfloat16)
        gelu_val, gelu_der = gelu_pair(pre_gate)
        up_f32 = pre_up.astype(jnp.float32)
        hidden = (gelu_val * up_f32).astype(jnp.bfloat16)
        grad_h = lax.dot_general(gy_all, out, ROW_DIMS, preferred_element_type=jnp.float32)
        grad_gate = (grad_h * up_f32 * gelu_der).astype(jnp.bfloat16)
        grad_up = (grad_h * gelu_val).astype(jnp.bfloat16)
        grad_x_part = lax.dot_general(grad_gate, gate, ROW_DIMS, preferred_element_type=jnp.float32) + lax.dot_general(grad_up, up, ROW_DIMS, preferred_element_type=jnp.float32)
        grad_x = lax.psum_scatter(grad_x_part, "row", scatter_dimension=0, tiled=True)
        grad_x = lax.psum_scatter(grad_x, "col", scatter_dimension=1, tiled=True).astype(jnp.bfloat16)
        dw_gate = lax.dot_general(x_all, grad_gate, COL_DIMS, preferred_element_type=jnp.float32)
        dw_gate = lax.all_to_all(dw_gate, "row", split_axis=0, concat_axis=1, tiled=True)
        dw_up = lax.dot_general(x_all, grad_up, COL_DIMS, preferred_element_type=jnp.float32)
        dw_up = lax.all_to_all(dw_up, "row", split_axis=0, concat_axis=1, tiled=True)
        dw_out = lax.dot_general(hidden, gy_all, COL_DIMS, preferred_element_type=jnp.float32)
        dw_out = lax.ppermute(dw_out, ("col", "row"), from_slice)
        dw_out = lax.all_to_all(dw_out, "col", split_axis=1, concat_axis=0, tiled=True)
        return grad_x, dw_gate, dw_up, dw_out

    return jax.shard_map(block_backward, mesh=mesh, in_specs=(act_spec, act_spec, weight_spec, weight_spec, weight_spec), out_specs=(act_spec, act_spec, act_spec, act_spec), check_vma=False)
```

```python
import functools
import math
import jax
import jax.numpy as jnp
from jax import lax
from jax.experimental import pallas as pl
from jax.experimental.pallas import tpu as pltpu
from jax.sharding import PartitionSpec as P

GELU_SCALE = math.sqrt(2.0 / math.pi)
ROW_DIMS = (((1,), (1,)), ((), ()))
COL_DIMS = (((0,), (0,)), ((), ()))
MESH = pl.DeviceIdType.MESH
ANY = pl.BlockSpec(memory_space=pl.ANY)
VMEM = pl.BlockSpec(memory_space=pltpu.VMEM)
VMEM_LIMIT = 64 * 1024 * 1024 - 65536


def gelu_pair(pre_act):
    pre_f32 = pre_act.astype(jnp.float32)
    inner_arg = GELU_SCALE * (pre_f32 + 0.044715 * pre_f32 * pre_f32 * pre_f32)
    tanh_val = jnp.tanh(inner_arg)
    gelu_val = 0.5 * pre_f32 * (1.0 + tanh_val)
    gelu_der = 0.5 * (1.0 + tanh_val) + 0.5 * pre_f32 * (1.0 - tanh_val * tanh_val) * GELU_SCALE * (1.0 + 3.0 * 0.044715 * pre_f32 * pre_f32)
    return gelu_val, gelu_der


class Place:
    def __init__(self):
        row, self.y = lax.axis_index("row"), lax.axis_index("col")
        self.row = row
        self.x, self.c = lax.div(row, 2), lax.rem(row, 2)
        self.other = 1 - self.c

    def xs(self, d):
        return lax.rem(self.x + (d % 4), 4)

    def ys(self, d):
        return lax.rem(self.y + (d % 4), 4)

    def to_x(self, d, core):
        return {"row": 2 * self.xs(d) + core, "col": self.y}

    def to_y(self, d):
        return {"row": self.row, "col": self.ys(d)}

    def partner(self):
        return {"row": 2 * self.x + self.other, "col": self.y}

    def barrier(self):
        sem = pltpu.get_barrier_semaphore()
        peers = [self.to_x(d, k) for d in (1, -1) for k in (0, 1)]
        peers += [self.to_y(1), self.to_y(-1), self.partner()]
        for peer in peers:
            pl.semaphore_signal(sem, inc=1, device_id=peer, device_id_type=MESH)
        pl.semaphore_wait(sem, len(peers))


class Net:
    def __init__(self, send_sem, recv_sem):
        self.send_sem, self.recv_sem = send_sem, recv_sem
        self.ids, self.sent = {}, []

    def copy(self, tag, src, dst, peer):
        i = self.ids.setdefault(tag, len(self.ids))
        return pltpu.make_async_remote_copy(
            src_ref=src, dst_ref=dst, send_sem=self.send_sem.at[i], recv_sem=self.recv_sem.at[i],
            device_id=peer, device_id_type=MESH)

    def send(self, tag, src, dst, peer):
        copy = self.copy(tag, src, dst, peer)
        copy.start()
        self.sent.append(copy)

    def arrived(self, tag, dst, peer):
        self.copy(tag, dst, dst, peer).wait_recv()

    def finish(self):
        for copy in self.sent:
            copy.wait_send()


def rows(ref, start, size):
    return ref.at[pl.ds(pl.multiple_of(start, size), size), :]


def cols(ref, start, size):
    return ref.at[:, pl.ds(pl.multiple_of(start, size), size)]


def block(ref, row, nr, col, nc):
    return ref.at[pl.ds(pl.multiple_of(row, nr), nr), pl.ds(pl.multiple_of(col, nc), nc)]


def gather_kernel(x_ref, gy_ref, wg_ref, wu_ref, wo_ref,
                  xg, yg, wgs, wus, wos, relay_w, mid, relay_o, relay_q,
                  bounce_w, bounce_o, bounce_q, send_sem, recv_sem, local_sem):
    at = Place()
    net = Net(send_sem, recv_sem)
    tb, db = x_ref.shape
    rb = wg_ref.shape[0]
    fs = wgs.shape[1]
    gath, own = (xg, yg), (x_ref, gy_ref)
    ws, wsrc = (wgs, wus), (wg_ref, wu_ref)
    here = at.partner()

    def blk(u, dx, dy, part=None):
        row, n = (2 * at.xs(dx) + at.c) * tb, tb
        if part is not None:
            row, n = row + part * (tb // 2), tb // 2
        return block(gath[u], row, n, at.ys(dy) * db, db)

    loads = []
    for w in (0, 1):
        loads.append(pltpu.make_async_copy(cols(wsrc[w], (4 * at.c + at.x) * fs, fs), bounce_w.at[w], local_sem.at[w]))
    loads.append(pltpu.make_async_copy(rows(wo_ref, at.x * fs, fs), bounce_o, local_sem.at[2]))
    for cp in loads:
        cp.start()
    at.barrier()

    def x_piece(xd, core):
        return (4 * core + at.xs(xd)) * fs

    for u in (0, 1):
        for d in (1, -1):
            net.send(("x", u, d), own[u], blk(u, 0, 0), at.to_x(d, at.c))
            net.send(("y", u, 0, d), own[u], blk(u, 0, 0), at.to_y(d))
    stores = []
    for u in (0, 1):
        stores.append(pltpu.make_async_copy(own[u], blk(u, 0, 0), local_sem.at[3 + u]))
        stores[-1].start()
    for d in (1, -1):
        net.send(("o", d), rows(wo_ref, at.xs(d) * fs, fs), mid.at[at.x], at.to_x(d, at.c))
        half = 0 if d == 1 else 1
        net.send(("or", d), rows(wo_ref, at.xs(2) * fs + half * (fs // 2), fs // 2), relay_o.at[half], at.to_x(d, at.c))
    for cp in loads:
        cp.wait()
    stores.append(pltpu.make_async_copy(bounce_o, mid.at[at.x], local_sem.at[2]))
    stores[-1].start()
    for w in (0, 1):
        stores.append(pltpu.make_async_copy(bounce_w.at[w], rows(ws[w], at.row * rb, rb), local_sem.at[w]))
        stores[-1].start()
    for w in (0, 1):
        mine = rows(ws[w], at.row * rb, rb)
        net.send(("wp", w), cols(wsrc[w], x_piece(0, at.other), fs), mine, at.partner())
        for d in (1, -1):
            half = 0 if d == 1 else 1
            far_core = at.c if d == 1 else at.other
            net.send(("wr", w, d), cols(wsrc[w], x_piece(2, far_core), fs), relay_w.at[w, half], at.to_x(d, at.c))
            for rel, core in ((0, at.c), (1, at.other)):
                net.send(("w", w, d, rel), cols(wsrc[w], x_piece(d, core), fs), mine, at.to_x(d, core))

    def forward_y(u, j, dx):
        for d in (1, -1):
            net.send(("y", u, j, d), blk(u, dx, 0), blk(u, dx, 0), at.to_y(d))

    def halves_y(u, j, dx):
        for d in (1, -1):
            half = 0 if d == 1 else 1
            net.arrived(("y", u, j, d), blk(u, dx, -d), here)
            net.send(("yh", u, j, d), blk(u, dx, -d, half), blk(u, dx, -d, half), at.to_y(d))

    def row_done(u, j, dx):
        for d in (1, -1):
            half = 0 if d == 1 else 1
            net.arrived(("yh", u, j, d), blk(u, dx, -2 * d, half), here)
        src = rows(gath[u], (2 * at.xs(dx) + at.c) * tb, tb)
        net.send(("p", u, j), src, src, at.partner())

    for u in (0, 1):
        for j, d in ((1, 1), (2, -1)):
            half = 0 if d == 1 else 1
            net.arrived(("x", u, d), blk(u, -d, 0), here)
            net.send(("xh", u, d), blk(u, -d, 0, half), blk(u, -d, 0, half), at.to_x(d, at.c))
            forward_y(u, j, -d)
    for cp in stores:
        cp.wait()
    for d in (1, -1):
        half = 0 if d == 1 else 1
        net.arrived(("or", d), relay_o.at[half], here)
        net.send(("of", d), relay_o.at[half], mid.at[at.xs(-d), pl.ds(half * (fs // 2), fs // 2), :], at.to_x(d, at.c))
    for u in (0, 1):
        halves_y(u, 0, 0)
    for d in (1, -1):
        half = 0 if d == 1 else 1
        net.arrived(("o", d), mid.at[at.xs(-d)], here)
        net.arrived(("of", d), mid.at[at.xs(-2 * d), pl.ds(half * (fs // 2), fs // 2), :], here)
    load = pltpu.make_async_copy(mid.at[at.y], bounce_q, local_sem.at[2])
    load.start()
    for d in (1, -1):
        half = 0 if d == 1 else 1
        net.send(("q", d), mid.at[at.ys(d)], cols(wos, at.y * db, db), at.to_y(d))
        net.send(("qr", d), mid.at[at.ys(2), pl.ds(half * (fs // 2), fs // 2), :], relay_q.at[half], at.to_y(d))
    load.wait()
    store = pltpu.make_async_copy(bounce_q, cols(wos, at.y * db, db), local_sem.at[2])
    store.start()
    for u in (0, 1):
        for d in (1, -1):
            half = 0 if d == 1 else 1
            net.arrived(("xh", u, d), blk(u, -2 * d, 0, half), here)
        forward_y(u, 3, 2)
    for w in (0, 1):
        for d in (1, -1):
            half = 0 if d == 1 else 1
            core = at.c if d == 1 else at.other
            net.arrived(("wr", w, d), relay_w.at[w, half], here)
            net.send(("wf", w, d), relay_w.at[w, half], rows(ws[w], (2 * at.xs(-d) + at.c) * rb, rb), at.to_x(d, core))
    for u in (0, 1):
        row_done(u, 0, 0)
    for d in (1, -1):
        half = 0 if d == 1 else 1
        net.arrived(("qr", d), relay_q.at[half], here)
        net.send(("qf", d), relay_q.at[half], block(wos, half * (fs // 2), fs // 2, at.ys(-d) * db, db), at.to_y(d))
    for j, dx in ((1, -1), (2, 1), (3, 2)):
        for u in (0, 1):
            halves_y(u, j, dx)
        for u in (0, 1):
            row_done(u, j, dx)
    for d in (1, -1):
        half = 0 if d == 1 else 1
        net.arrived(("q", d), cols(wos, at.ys(-d) * db, db), here)
        net.arrived(("qf", d), block(wos, half * (fs // 2), fs // 2, at.ys(-2 * d) * db, db), here)
    for w in (0, 1):
        net.arrived(("wp", w), rows(ws[w], (2 * at.x + at.other) * rb, rb), here)
        for d in (1, -1):
            for rel, core in ((0, at.c), (1, at.other)):
                net.arrived(("w", w, d, rel), rows(ws[w], (2 * at.xs(-d) + core) * rb, rb), here)
            core = at.c if d == 1 else at.other
            net.arrived(("wf", w, d), rows(ws[w], (2 * at.xs(-2 * d) + core) * rb, rb), here)
    for j, dx in ((0, 0), (1, -1), (2, 1), (3, 2)):
        for u in (0, 1):
            net.arrived(("p", u, j), rows(gath[u], (2 * at.xs(dx) + at.other) * tb, tb), here)
    store.wait()
    net.finish()


def scatter_kernel(dxp, dg, du, do, dx_out, dg_out, du_out, do_out, relay_w, mid, relay_q, relay_o,
                   part, own, yh, yf, xh, xf, bounce_w, bounce_o, send_sem, recv_sem, local_sem):
    at = Place()
    net = Net(send_sem, recv_sem)
    tb, db = dx_out.shape
    rb = dg_out.shape[0]
    fs = dg.shape[1]
    hb = tb // 2
    wsrc, ws = (dg, du), (dg_out, du_out)
    here = at.partner()
    order = (2, 1, -1, 0)

    def own_rows(dx, core):
        return rows(dxp, (2 * at.xs(dx) + core) * tb, tb)

    loads = []
    for w in (0, 1):
        loads.append(pltpu.make_async_copy(rows(wsrc[w], at.row * rb, rb), bounce_w.at[w], local_sem.at[w]))
    loads.append(pltpu.make_async_copy(cols(do, at.y * db, db), bounce_o.at[0], local_sem.at[2]))
    for cp in loads:
        cp.start()
    own_loads = [pltpu.make_async_copy(own_rows(dx, at.c), own.at[j % 2], local_sem.at[4 + j % 2]) for j, dx in enumerate(order)]
    own_loads[0].start()
    own_loads[1].start()
    at.barrier()
    for j, dx in enumerate(order):
        net.send(("p", j), own_rows(dx, at.other), part.at[j], at.partner())
    for d in (1, -1):
        half = 0 if d == 1 else 1
        net.send(("qr", d), block(do, half * (fs // 2), fs // 2, at.ys(2) * db, db), relay_q.at[half], at.to_y(d))
        net.send(("q", d), cols(do, at.ys(d) * db, db), mid.at[at.y], at.to_y(d))
    for w in (0, 1):
        mine = cols(ws[w], (4 * at.c + at.x) * fs, fs)

        def piece(xd, core):
            return rows(wsrc[w], (2 * at.xs(xd) + core) * rb, rb)

        for d in (1, -1):
            half = 0 if d == 1 else 1
            far_core = at.c if d == 1 else at.other
            net.send(("wr", w, d), piece(2, far_core), relay_w.at[w, half], at.to_x(d, at.c))
        for d in (1, -1):
            for rel, core in ((0, at.c), (1, at.other)):
                net.send(("w", w, d, rel), piece(d, core), mine, at.to_x(d, core))
        net.send(("wp", w), piece(0, at.other), mine, at.partner())
    for cp in loads:
        cp.wait()
    stores = [pltpu.make_async_copy(bounce_w.at[w], cols(ws[w], (4 * at.c + at.x) * fs, fs), local_sem.at[w]) for w in (0, 1)]
    stores.append(pltpu.make_async_copy(bounce_o.at[0], mid.at[at.y], local_sem.at[2]))
    for cp in stores:
        cp.start()

    def y_cols(d):
        return pl.ds(pl.multiple_of(at.ys(d) * db, db), db)

    for j, dx in enumerate(order):
        net.arrived(("p", j), part.at[j], here)
        own_loads[j].wait()
        part[j] = part[j] + own[j % 2]
        if j + 2 < 4:
            own_loads[j + 2].start()
        for d in (1, -1):
            half = 0 if d == 1 else 1
            net.send(("yh", j, d), part.at[j, pl.ds(half * hb, hb), y_cols(2)], yh.at[j, half], at.to_y(d))
    for cp in stores:
        cp.wait()
    for d in (1, -1):
        half = 0 if d == 1 else 1
        net.arrived(("qr", d), relay_q.at[half], here)
        net.send(("qf", d), relay_q.at[half], mid.at[at.ys(-d), pl.ds(half * (fs // 2), fs // 2), :], at.to_y(d))
    for w in (0, 1):
        for d in (1, -1):
            half = 0 if d == 1 else 1
            core = at.c if d == 1 else at.other
            net.arrived(("wr", w, d), relay_w.at[w, half], here)
            src_piece = (4 * at.c + at.xs(-d)) * fs
            net.send(("wf", w, d), relay_w.at[w, half], cols(ws[w], src_piece, fs), at.to_x(d, core))
    for j, dx in enumerate(order):
        for d in (1, -1):
            half = 0 if d == 1 else 1
            net.arrived(("yh", j, d), yh.at[j, half], here)
            here_rows = pl.ds(half * hb, hb)
            part[j, here_rows, y_cols(d)] = part[j, here_rows, y_cols(d)] + yh[j, half]
            net.send(("yf", j, d), part.at[j, :, y_cols(d)], yf.at[j, half], at.to_y(d))
    for d in (1, -1):
        half = 0 if d == 1 else 1
        net.arrived(("q", d), mid.at[at.ys(-d)], here)
        net.arrived(("qf", d), mid.at[at.ys(-2 * d), pl.ds(half * (fs // 2), fs // 2), :], here)
    load = pltpu.make_async_copy(mid.at[at.x], bounce_o.at[1], local_sem.at[2])
    load.start()
    for d in (1, -1):
        half = 0 if d == 1 else 1
        net.send(("or", d), mid.at[at.xs(2), pl.ds(half * (fs // 2), fs // 2), :], relay_o.at[half], at.to_x(d, at.c))
    for d in (1, -1):
        net.send(("o", d), mid.at[at.xs(d)], rows(do_out, at.x * fs, fs), at.to_x(d, at.c))
    load.wait()
    store = pltpu.make_async_copy(bounce_o.at[1], rows(do_out, at.x * fs, fs), local_sem.at[2])
    store.start()
    for j, dx in enumerate(order):
        for d in (1, -1):
            half = 0 if d == 1 else 1
            net.arrived(("yf", j, d), yf.at[j, half], here)
        yf[j, 0] = yf[j, 0] + yf[j, 1] + part[j, :, y_cols(0)]
        if j == 0:
            for d in (1, -1):
                half = 0 if d == 1 else 1
                net.send(("xh", d), yf.at[0, 0, pl.ds(half * hb, hb), :], xh.at[half], at.to_x(d, at.c))
    for d in (1, -1):
        half = 0 if d == 1 else 1
        net.arrived(("or", d), relay_o.at[half], here)
        net.send(("of", d), relay_o.at[half], block(do_out, at.xs(-d) * fs + half * (fs // 2), fs // 2, 0, db), at.to_x(d, at.c))
    for d in (1, -1):
        half, j = (0, 1) if d == 1 else (1, 2)
        net.arrived(("xh", d), xh.at[half], here)
        here_rows = pl.ds(half * hb, hb)
        yf[j, 0, here_rows, :] = yf[j, 0, here_rows, :] + xh[half]
        net.send(("xf", d), yf.at[j, 0], xf.at[half], at.to_x(d, at.c))
    for d in (1, -1):
        half = 0 if d == 1 else 1
        net.arrived(("xf", d), xf.at[half], here)
    dx_out[...] = (yf[3, 0] + xf[0] + xf[1]).astype(dx_out.dtype)
    for d in (1, -1):
        half = 0 if d == 1 else 1
        net.arrived(("o", d), rows(do_out, at.xs(-d) * fs, fs), here)
        net.arrived(("of", d), block(do_out, at.xs(-2 * d) * fs + half * (fs // 2), fs // 2, 0, db), here)
    for w in (0, 1):
        net.arrived(("wp", w), cols(ws[w], (4 * at.other + at.x) * fs, fs), here)
        for d in (1, -1):
            for rel, core in ((0, at.c), (1, at.other)):
                net.arrived(("w", w, d, rel), cols(ws[w], (4 * core + at.xs(-d)) * fs, fs), here)
            core = at.c if d == 1 else at.other
            net.arrived(("wf", w, d), cols(ws[w], (4 * core + at.xs(-2 * d)) * fs, fs), here)
    store.wait()
    net.finish()


def gather(x_blk, gy_blk, gate_blk, up_blk, out_blk):
    (tb, db), (rb, fcol) = x_blk.shape, gate_blk.shape
    t, d, fs = 8 * tb, 4 * db, fcol // 8
    bf = jnp.bfloat16
    outs = [(t, d), (t, d), (d, fs), (d, fs), (fs, d),
            (2, 2, rb, fs), (4, fs, db), (2, fs // 2, db), (2, fs // 2, db)]
    got = pl.pallas_call(
        gather_kernel,
        name="gather_inputs",
        out_shape=[jax.ShapeDtypeStruct(s, bf) for s in outs],
        in_specs=[VMEM, VMEM, ANY, ANY, ANY],
        out_specs=[ANY] * len(outs),
        scratch_shapes=[
            pltpu.VMEM((2, rb, fs), bf), pltpu.VMEM((fs, db), bf), pltpu.VMEM((fs, db), bf),
            pltpu.SemaphoreType.DMA((80,)), pltpu.SemaphoreType.DMA((80,)), pltpu.SemaphoreType.DMA((5,)),
        ],
        compiler_params=pltpu.CompilerParams(collective_id=0, has_side_effects=True),
    )(x_blk, gy_blk, gate_blk, up_blk, out_blk)
    return got[:5]


def scatter(dxp, dg, du, do, like_x, like_w):
    (tb, db), (rb, fcol) = like_x.shape, like_w.shape
    fs = fcol // 8
    f32 = jnp.float32
    outs = [((tb, db), jnp.bfloat16), ((rb, fcol), f32), ((rb, fcol), f32), ((4 * fs, db), f32),
            ((2, 2, rb, fs), f32), ((4, fs, db), f32), ((2, fs // 2, db), f32), ((2, fs // 2, db), f32)]
    got = pl.pallas_call(
        scatter_kernel,
        name="scatter_results",
        out_shape=[jax.ShapeDtypeStruct(*s) for s in outs],
        in_specs=[ANY] * 4,
        out_specs=[VMEM] + [ANY] * (len(outs) - 1),
        scratch_shapes=[
            pltpu.VMEM((4, tb, 4 * db), f32), pltpu.VMEM((2, tb, 4 * db), f32),
            pltpu.VMEM((4, 2, tb // 2, db), f32), pltpu.VMEM((4, 2, tb, db), f32),
            pltpu.VMEM((2, tb // 2, db), f32), pltpu.VMEM((2, tb, db), f32),
            pltpu.VMEM((2, rb, fs), f32), pltpu.VMEM((2, fs, db), f32),
            pltpu.SemaphoreType.DMA((64,)), pltpu.SemaphoreType.DMA((64,)), pltpu.SemaphoreType.DMA((6,)),
        ],
        compiler_params=pltpu.CompilerParams(collective_id=1, has_side_effects=True, vmem_limit_bytes=VMEM_LIMIT),
    )(dxp, dg, du, do)
    return got[:4]


def solution(mesh):
    act_spec = P(("dp", "row"), "col")
    weight_spec = P("row", "col")
    assert mesh.shape["row"] == 8 and mesh.shape["col"] == 4

    def block_backward(x_blk, gy_blk, gate_blk, up_blk, out_blk):
        x_all, gy_all, gate, up, out = gather(x_blk, gy_blk, gate_blk, up_blk, out_blk)
        pre_gate = jnp.dot(x_all, gate, preferred_element_type=jnp.float32).astype(jnp.bfloat16)
        pre_up = jnp.dot(x_all, up, preferred_element_type=jnp.float32).astype(jnp.bfloat16)
        gelu_val, gelu_der = gelu_pair(pre_gate)
        up_f32 = pre_up.astype(jnp.float32)
        hidden = (gelu_val * up_f32).astype(jnp.bfloat16)
        grad_h = lax.dot_general(gy_all, out, ROW_DIMS, preferred_element_type=jnp.float32)
        grad_gate = (grad_h * up_f32 * gelu_der).astype(jnp.bfloat16)
        grad_up = (grad_h * gelu_val).astype(jnp.bfloat16)
        grad_x_part = lax.dot_general(grad_gate, gate, ROW_DIMS, preferred_element_type=jnp.float32) + lax.dot_general(grad_up, up, ROW_DIMS, preferred_element_type=jnp.float32)
        dw_gate = lax.dot_general(x_all, grad_gate, COL_DIMS, preferred_element_type=jnp.float32)
        dw_up = lax.dot_general(x_all, grad_up, COL_DIMS, preferred_element_type=jnp.float32)
        dw_out = lax.dot_general(hidden, gy_all, COL_DIMS, preferred_element_type=jnp.float32)
        return tuple(scatter(grad_x_part, dw_gate, dw_up, dw_out, x_blk, gate_blk))

    return jax.shard_map(block_backward, mesh=mesh, in_specs=(act_spec, act_spec, weight_spec, weight_spec, weight_spec), out_specs=(act_spec, act_spec, act_spec, act_spec), check_vma=False)
```
